8 devices in a mesh: dp: 1 (over z), ep: 8 (over y, x, core).
Axes of the slice: x: 2, y: 2, z: 1, core: 2. Of those that a mesh axis runs over, the one named last changes fastest.
Arguments:
- hidden_in: bfloat16 [2048, 2560], P(('dp', 'ep'))
- norm_gain: float32 [2560], replicated
- router_w: float32 [64, 2560], replicated
- w_gate: bfloat16 [64, 2560, 1536], P('ep')
- w_up: bfloat16 [64, 2560, 1536], P('ep')
- w_down: bfloat16 [64, 1536, 2560], P('ep')
- ws_gate: bfloat16 [2560, 3072], replicated
- ws_up: bfloat16 [2560, 3072], replicated
- ws_down: bfloat16 [3072, 2560], replicated
- expert_ids: int32 [2048, 6], P(('dp', 'ep'))
Outputs:
- output: bfloat16 [2048, 2560], P(('dp', 'ep'))
All inputs are finite; a program needn't handle non-finite values.
Results may differ from the reference program's by a relative error of at most 0.00440109.
Values are sent between devices in bfloat16 or wider.
A program may use at most 1 GiB of HBM per device.

```python
import jax
import jax.numpy as jnp
from jax import lax

TOKENS = 2048
D = 2560
EXPERTS = 64
INTER = 1536
SHARED_INTER = 3072
TOP = 6
GROUPS = 8
GROUP_LIMIT = 4

NORM_EPS = 1e-6
ROUTE_SCALE = 2.5
GROUP_WIDTH = EXPERTS // GROUPS
SLOT_PAIRS = (TOP + GROUP_LIMIT - 1) // GROUP_LIMIT
EXP_CAP = GROUPS * SLOT_PAIRS * TOKENS // EXPERTS


def draw_routes(route_key):
    key_hot, key_other, key_shift, key_cols = jax.random.split(route_key, 4)
    slot_sizes = [TOP // GROUP_LIMIT + int(slot_num < TOP % GROUP_LIMIT) for slot_num in range(GROUP_LIMIT)]
    slot_of_pair = jnp.array([slot_num for slot_num in range(GROUP_LIMIT) for step_num in range(slot_sizes[slot_num])], jnp.int32)
    step_of_pair = jnp.array([step_num for slot_num in range(GROUP_LIMIT) for step_num in range(slot_sizes[slot_num])], jnp.int32)
    hot_group = jax.random.randint(key_hot, (), 0, GROUPS).astype(jnp.int32)
    other_scores = jax.random.randint(key_other, (TOKENS, GROUPS - 1), 0, 1 << 20).astype(jnp.int32) * (GROUPS - 1) + jnp.arange(GROUPS - 1, dtype=jnp.int32)
    other_offsets = jnp.argsort(other_scores, axis=1)[:, : GROUP_LIMIT - 1].astype(jnp.int32)
    token_groups = jnp.concatenate([jnp.zeros((TOKENS, 1), jnp.int32) + hot_group, (hot_group + 1 + other_offsets) % GROUPS], axis=1)
    pair_groups = token_groups[:, slot_of_pair]
    group_shift = jax.random.randint(key_shift, (GROUPS,), 0, GROUP_WIDTH).astype(jnp.int32)
    token_pos = jnp.arange(TOKENS, dtype=jnp.int32)[:, None]
    within = (token_pos + step_of_pair[None, :] + group_shift[pair_groups]) % GROUP_WIDTH
    routes = pair_groups * GROUP_WIDTH + within
    col_scores = jax.random.randint(key_cols, (TOKENS, TOP), 0, 1 << 20).astype(jnp.int32) * TOP + jnp.arange(TOP, dtype=jnp.int32)
    col_order = jnp.argsort(col_scores, axis=1)
    return jnp.take_along_axis(routes, col_order, axis=1).astype(jnp.int32)


def setup_inputs(seed: int = 0, part: int = 0) -> dict:
    base_key = jax.random.key(seed)
    weight_keys = jax.random.split(base_key, 9)
    part_keys = jax.random.split(jax.random.fold_in(base_key, part), 2)
    hidden_in = jax.random.normal(part_keys[0], (TOKENS, D), jnp.float32).astype(jnp.bfloat16)
    expert_ids = draw_routes(part_keys[1])
    norm_gain = jax.random.uniform(weight_keys[0], (D,), jnp.float32, 0.5, 1.5)
    router_w = jax.random.normal(weight_keys[1], (EXPERTS, D), jnp.float32) * D ** -0.5
    w_gate = (jax.random.normal(weight_keys[2], (EXPERTS, D, INTER), jnp.float32) * D ** -0.5).astype(jnp.bfloat16)
    w_up = (jax.random.normal(weight_keys[3], (EXPERTS, D, INTER), jnp.float32) * D ** -0.5).astype(jnp.bfloat16)
    out_scale = jax.random.uniform(weight_keys[4], (EXPERTS, 1, 1), jnp.float32, 1.0, 3.0)
    w_down = (jax.random.normal(weight_keys[5], (EXPERTS, INTER, D), jnp.float32) * INTER ** -0.5 * out_scale).astype(jnp.bfloat16)
    ws_gate = (jax.random.normal(weight_keys[6], (D, SHARED_INTER), jnp.float32) * D ** -0.5).astype(jnp.bfloat16)
    ws_up = (jax.random.normal(weight_keys[7], (D, SHARED_INTER), jnp.float32) * D ** -0.5).astype(jnp.bfloat16)
    ws_down = (jax.random.normal(weight_keys[8], (SHARED_INTER, D), jnp.float32) * SHARED_INTER ** -0.5).astype(jnp.bfloat16)
    return {"hidden_in": hidden_in, "norm_gain": norm_gain, "router_w": router_w, "w_gate": w_gate, "w_up": w_up, "w_down": w_down, "ws_gate": ws_gate, "ws_up": ws_up, "ws_down": ws_down, "expert_ids": expert_ids}


def swiglu(tok_rows, gate_mat, up_mat, down_mat):
    h_gate = jnp.dot(tok_rows, gate_mat, preferred_element_type=jnp.float32)
    h_up = jnp.dot(tok_rows, up_mat, preferred_element_type=jnp.float32)
    hidden = (jax.nn.silu(h_gate) * h_up).astype(jnp.bfloat16)
    return jnp.dot(hidden, down_mat, preferred_element_type=jnp.float32).astype(jnp.bfloat16)


def reference(hidden_in, norm_gain, router_w, w_gate, w_up, w_down, ws_gate, ws_up, ws_down, expert_ids):
    x_f32 = hidden_in.astype(jnp.float32)
    inv_rms = lax.rsqrt(jnp.mean(x_f32 * x_f32, axis=1, keepdims=True) + NORM_EPS)
    x_norm = (x_f32 * inv_rms * norm_gain).astype(jnp.bfloat16)
    scores = jax.nn.sigmoid(jnp.dot(x_norm.astype(jnp.float32), router_w.T))
    picked = jnp.take_along_axis(scores, expert_ids, axis=1)
    gate_vals = ROUTE_SCALE * picked / jnp.sum(picked, axis=1, keepdims=True)
    flat_ids = expert_ids.reshape(-1)
    pair_tok = jnp.arange(TOKENS * TOP, dtype=jnp.int32) // TOP
    sort_order = jnp.argsort(flat_ids)
    counts = jnp.bincount(flat_ids, length=EXPERTS).astype(jnp.int32)
    starts = jnp.cumsum(counts) - counts
    sorted_tok = jnp.concatenate([pair_tok[sort_order], jnp.full((EXP_CAP,), TOKENS, jnp.int32)])
    norm_pad = jnp.concatenate([x_norm, jnp.zeros((1, D), x_norm.dtype)], axis=0)

    def one_expert(expert_xs):
        gate_mat, up_mat, down_mat, row_start, row_count = expert_xs
        row_tok = lax.dynamic_slice(sorted_tok, (row_start,), (EXP_CAP,))
        row_tok = jnp.where(jnp.arange(EXP_CAP, dtype=jnp.int32) < row_count, row_tok, TOKENS)
        return swiglu(norm_pad[row_tok], gate_mat, up_mat, down_mat)

    expert_out = lax.map(one_expert, (w_gate, w_up, w_down, starts, counts))
    sorted_rank = (jnp.arange(TOKENS * TOP, dtype=jnp.int32) - starts[flat_ids[sort_order]]).astype(jnp.int32)
    pair_rank = jnp.zeros((TOKENS * TOP,), jnp.int32).at[sort_order].set(sorted_rank)
    pair_out = expert_out[flat_ids, pair_rank].reshape(TOKENS, TOP, D)
    routed = jnp.sum(gate_vals[:, :, None] * pair_out.astype(jnp.float32), axis=1)
    shared_out = swiglu(x_norm, ws_gate, ws_up, ws_down)
    return (x_f32 + shared_out.astype(jnp.float32) + routed).astype(jnp.bfloat16)
```

```python
import functools

import jax
import jax.numpy as jnp
from jax import lax
from jax.experimental import pallas as pl
from jax.experimental.pallas import tpu as pltpu
from jax.sharding import PartitionSpec as P

NORM_EPS = 1e-6
ROUTE_SCALE = 2.5
LANES = 128
MESH = pl.DeviceIdType.MESH
VMEM_LIMIT = 66_000_000


def rms_norm(x_rows, norm_gain):
    x_f32 = x_rows.astype(jnp.float32)
    inv_rms = lax.rsqrt(jnp.mean(x_f32 * x_f32, axis=-1, keepdims=True) + NORM_EPS)
    return (x_f32 * inv_rms * norm_gain).astype(jnp.bfloat16)


def route_gates(x_norm, router_w, expert_ids):
    logits = jnp.einsum("td,nd->tn", x_norm.astype(jnp.float32), router_w, precision=lax.Precision.HIGHEST, preferred_element_type=jnp.float32)
    scores = jax.nn.sigmoid(logits)
    hot = expert_ids[:, :, None] == jnp.arange(router_w.shape[0], dtype=jnp.int32)[None, None, :]
    picked = jnp.sum(jnp.where(hot, scores[:, None, :], 0.0), axis=2)
    return ROUTE_SCALE * picked / jnp.sum(picked, axis=1, keepdims=True)


def swiglu(tok_rows, gate_mat, up_mat, down_mat):
    h_gate = jnp.dot(tok_rows, gate_mat, preferred_element_type=jnp.float32)
    h_up = jnp.dot(tok_rows, up_mat, preferred_element_type=jnp.float32)
    hidden = (jax.nn.silu(h_gate) * h_up).astype(jnp.bfloat16)
    return jnp.dot(hidden, down_mat, preferred_element_type=jnp.float32).astype(jnp.bfloat16)


def gate_up_kernel(tok_ref, xn_ref, wg_ref, wu_ref, h_ref, xf, gbuf, lhs):
    e = pl.program_id(0)
    j = pl.program_id(1)
    cap, d = lhs.shape
    nc = d // LANES

    @pl.when((e == 0) & (j == 0))
    def _():
        def widen(b, _):
            rows = pl.multiple_of(b * 64, 64)
            blk = xn_ref[pl.ds(rows, 64), :].astype(jnp.float32)
            for c in range(nc):
                xf[pl.ds(rows * nc + c, 64, stride=nc), :] = blk[:, c * LANES:(c + 1) * LANES]
            return 0
        lax.fori_loop(0, xn_ref.shape[0] // 64, widen, 0)

    @pl.when(j == 0)
    def _():
        def gather(b, _):
            for u in range(16):
                r = b * 16 + u
                gbuf[pl.ds(r * nc, nc), :] = xf[pl.ds(tok_ref[e * cap + r], nc), :]
            return 0
        lax.fori_loop(0, cap // 16, gather, 0)

        def narrow(b, _):
            rows = pl.multiple_of(b * 64, 64)
            for c in range(nc):
                lhs[pl.ds(rows, 64), c * LANES:(c + 1) * LANES] = gbuf[pl.ds(rows * nc + c, 64, stride=nc), :].astype(jnp.bfloat16)
            return 0
        lax.fori_loop(0, cap // 64, narrow, 0)

    g = jnp.dot(lhs[...], wg_ref[0], preferred_element_type=jnp.float32)
    u = jnp.dot(lhs[...], wu_ref[0], preferred_element_type=jnp.float32)
    h_ref[0] = (g * jax.nn.sigmoid(g) * u).astype(jnp.bfloat16)


def gate_up(tok_off, xn_all, w_gate, w_up, block=512):
    n_exp, d, inter = w_gate.shape
    cap = tok_off.shape[0] // n_exp
    tokens = xn_all.shape[0]
    return pl.pallas_call(
        gate_up_kernel,
        grid_spec=pltpu.PrefetchScalarGridSpec(
            num_scalar_prefetch=1,
            grid=(n_exp, inter // block),
            in_specs=[
                pl.BlockSpec((tokens, d), lambda e, j, t: (0, 0), pipeline_mode=pl.Buffered(1)),
                pl.BlockSpec((1, d, block), lambda e, j, t: (e, 0, j)),
                pl.BlockSpec((1, d, block), lambda e, j, t: (e, 0, j)),
            ],
            out_specs=pl.BlockSpec((1, cap, block), lambda e, j, t: (e, 0, j)),
            scratch_shapes=[
                pltpu.VMEM((tokens * d // LANES, LANES), jnp.float32),
                pltpu.VMEM((cap * d // LANES, LANES), jnp.float32),
                pltpu.VMEM((cap, d), jnp.bfloat16),
            ],
        ),
        out_shape=jax.ShapeDtypeStruct((n_exp, cap, inter), jnp.bfloat16),
        compiler_params=pltpu.CompilerParams(vmem_limit_bytes=VMEM_LIMIT, dimension_semantics=("arbitrary", "arbitrary")),
        cost_estimate=pl.CostEstimate(flops=4 * n_exp * cap * d * inter, bytes_accessed=4 * n_exp * d * inter, transcendentals=0),
        name="gate_up",
    )(tok_off, xn_all, w_gate, w_up)


def neighbours():
    me = lax.axis_index("ep")
    core, bx, by = lax.rem(me, 2), lax.rem(me // 2, 2), me // 4
    return core, bx, by, me + 1 - 2 * core, me + 2 - 4 * bx, me + 4 - 8 * by


def down_kernel(cw, slot_ref, h_hbm, wd_hbm, gate_ref, base_ref, out_ref,
                h, wd, ybuf, part, got_core, got_x, got_y, got_xy, got_yx,
                h_sem, wd_sem, send_core, recv_core, send_x, recv_x, send_y, recv_y, send_2, recv_2):
    n_exp, cap, inter = h.shape
    d = base_ref.shape[1]
    n_chunk, sub = d // cw, cw // LANES
    rows = part.shape[2] // 2
    tok_dev = part.shape[2] // sub
    n_dev = 8
    top = 6
    core, bx, by, partner, xdev, ydev = neighbours()

    barrier = pltpu.get_barrier_semaphore()
    for dev in (partner, xdev, ydev):
        pl.semaphore_signal(barrier, inc=1, device_id={"ep": dev}, device_id_type=MESH)

    def h_copy(e):
        return pltpu.make_async_copy(h_hbm.at[e], h.at[e], h_sem.at[e])

    def wd_copy(s):
        c, e = s // n_exp, lax.rem(s, n_exp)
        slot = lax.rem(s, 3)
        return pltpu.make_async_copy(wd_hbm.at[e, :, pl.ds(pl.multiple_of(c * cw, LANES), cw)], wd.at[slot], wd_sem.at[slot])

    for e in range(n_exp):
        h_copy(e).start()
    n_step = n_chunk * n_exp
    wd_copy(0).start()
    wd_copy(1).start()
    ybuf[pl.ds(n_exp * cap * sub, 8), :] = jnp.zeros((8, LANES), jnp.float32)
    pl.semaphore_wait(barrier, 3)

    def remote(src, dst, send, recv, dev):
        return pltpu.make_async_remote_copy(src_ref=src, dst_ref=dst, send_sem=send, recv_sem=recv, device_id={"ep": dev}, device_id_type=MESH)

    def copy_core(c):
        p = lax.rem(c, 2)
        return [remote(part.at[p, 2 * q + 1 - core], got_core.at[c, q], send_core.at[p, q], recv_core.at[c, q], partner) for q in range(4)]

    def copy_x(c):
        return [remote(got_core.at[c, 2 * yy + 1 - bx, pl.ds(0, rows)], got_x.at[c, yy], send_x.at[c, yy], recv_x.at[c, yy], xdev) for yy in range(2)]

    def copy_y(c):
        return [remote(got_core.at[c, 2 * (1 - by) + xx, pl.ds(rows, rows)], got_y.at[c, xx], send_y.at[c, xx], recv_y.at[c, xx], ydev) for xx in range(2)]

    def copy_2(c):
        return [
            remote(got_core.at[c, 2 * (1 - by) + bx, pl.ds(0, rows)], got_xy.at[c], send_2.at[c, 0], recv_2.at[c, 0], ydev),
            remote(got_core.at[c, 2 * by + 1 - bx, pl.ds(rows, rows)], got_yx.at[c], send_2.at[c, 1], recv_2.at[c, 1], xdev),
        ]

    def add_into(dst, src, n):
        def one(i, _):
            at = pl.ds(pl.multiple_of(i * 64, 64), 64)
            dst[at, :] = dst[at, :] + src[at, :]
            return 0
        lax.fori_loop(0, n // 64, one, 0)

    def on_core(c):
        p = lax.rem(c, 2)
        for q, cp in enumerate(copy_core(c)):
            cp.wait_recv()
            add_into(got_core.at[c, q], part.at[p, 2 * q + core], 2 * rows)
        for cp in copy_x(c) + copy_y(c):
            cp.start()

    def on_first(c):
        for yy, cp in enumerate(copy_x(c)):
            cp.wait_recv()
            add_into(got_core.at[c, 2 * yy + bx, pl.ds(0, rows)], got_x.at[c, yy], rows)
        for xx, cp in enumerate(copy_y(c)):
            cp.wait_recv()
            add_into(got_core.at[c, 2 * by + xx, pl.ds(rows, rows)], got_y.at[c, xx], rows)
        for cp in copy_2(c):
            cp.start()

    def on_second(c):
        a, b = copy_2(c)
        mine = got_core.at[c, 2 * by + bx]
        a.wait_recv()
        add_into(mine.at[pl.ds(0, rows)], got_xy.at[c], rows)
        b.wait_recv()
        add_into(mine.at[pl.ds(rows, rows)], got_yx.at[c], rows)

    def down(c, lo, hi):
        def one(e, _):
            s = c * n_exp + e
            slot = lax.rem(s, 3)
            @pl.when(s + 2 < n_step)
            def _():
                wd_copy(s + 2).start()
            @pl.when(c == 0)
            def _():
                h_copy(e).wait()
            wd_copy(s).wait()
            y = jnp.dot(h[e], wd[slot], preferred_element_type=jnp.float32)
            y = y.astype(jnp.bfloat16).astype(jnp.float32) * gate_ref[e]
            for i in range(sub):
                ybuf[pl.ds(e * (cap * sub) + i, cap, stride=sub), :] = y[:, i * LANES:(i + 1) * LANES]
            return 0
        lax.fori_loop(lo, hi, one, 0)

    def combine(c):
        p = lax.rem(c, 2)
        def dev_loop(dev, _):
            def one(b, _):
                for u in range(8):
                    t = b * 8 + u
                    acc = None
                    for k in range(top):
                        row = ybuf[pl.ds(slot_ref[(dev * tok_dev + t) * top + k], sub), :]
                        acc = row if acc is None else acc + row
                    part[p, dev, pl.ds(t * sub, sub), :] = acc
                return 0
            lax.fori_loop(0, tok_dev // 8, one, 0)
            return 0
        lax.fori_loop(0, n_dev, dev_loop, 0)

    def chunk(c, _):
        down(c, 0, n_exp // 2)
        @pl.when(c >= 2)
        def _():
            on_first(c - 2)
        @pl.when(c >= 1)
        def _():
            on_core(c - 1)
        down(c, n_exp // 2, n_exp)
        @pl.when(c >= 2)
        def _():
            for cp in copy_core(c - 2):
                cp.wait_send()
        combine(c)
        for cp in copy_core(c):
            cp.start()
        return 0

    lax.fori_loop(0, n_chunk, chunk, 0)
    on_first(n_chunk - 2)
    on_core(n_chunk - 1)
    on_first(n_chunk - 1)

    def finish(c, _):
        on_second(c)
        for i in range(sub):
            at = pl.ds(pl.multiple_of(c * cw + i * LANES, LANES), LANES)
            routed = got_core[c, 2 * by + bx, pl.ds(i, tok_dev, stride=sub), :]
            out_ref[:, at] = (base_ref[:, at] + routed).astype(out_ref.dtype)
        for cp in copy_x(c) + copy_y(c) + copy_2(c):
            cp.wait_send()
        return 0
    lax.fori_loop(0, n_chunk, finish, 0)
    for c in (n_chunk - 2, n_chunk - 1):
        for cp in copy_core(c):
            cp.wait_send()


def down_reduce(slot_off, hidden, w_down, gate_col, base, cw=512):
    n_exp, cap, inter = hidden.shape
    tok_dev, d = base.shape
    sub, n_chunk = cw // LANES, d // cw
    blk = tok_dev * sub
    f32 = jnp.float32
    return pl.pallas_call(
        functools.partial(down_kernel, cw),
        out_shape=jax.ShapeDtypeStruct((tok_dev, d), jnp.bfloat16),
        in_specs=[
            pl.BlockSpec(memory_space=pltpu.SMEM),
            pl.BlockSpec(memory_space=pl.ANY),
            pl.BlockSpec(memory_space=pl.ANY),
            pl.BlockSpec(memory_space=pltpu.VMEM),
            pl.BlockSpec(memory_space=pltpu.VMEM),
        ],
        out_specs=pl.BlockSpec(memory_space=pltpu.VMEM),
        scratch_shapes=[
            pltpu.VMEM((n_exp, cap, inter), jnp.bfloat16),
            pltpu.VMEM((3, inter, cw), jnp.bfloat16),
            pltpu.VMEM((n_exp * cap * sub + 8, LANES), f32),
            pltpu.VMEM((2, 8, blk, LANES), f32),
            pltpu.VMEM((n_chunk, 4, blk, LANES), f32),
            pltpu.VMEM((n_chunk, 2, blk // 2, LANES), f32),
            pltpu.VMEM((n_chunk, 2, blk // 2, LANES), f32),
            pltpu.VMEM((n_chunk, blk // 2, LANES), f32),
            pltpu.VMEM((n_chunk, blk // 2, LANES), f32),
            pltpu.SemaphoreType.DMA((n_exp,)),
            pltpu.SemaphoreType.DMA((3,)),
            pltpu.SemaphoreType.DMA((2, 4)),
            pltpu.SemaphoreType.DMA((n_chunk, 4)),
            pltpu.SemaphoreType.DMA((n_chunk, 2)),
            pltpu.SemaphoreType.DMA((n_chunk, 2)),
            pltpu.SemaphoreType.DMA((n_chunk, 2)),
            pltpu.SemaphoreType.DMA((n_chunk, 2)),
            pltpu.SemaphoreType.DMA((n_chunk, 2)),
            pltpu.SemaphoreType.DMA((n_chunk, 2)),
        ],
        compiler_params=pltpu.CompilerParams(vmem_limit_bytes=VMEM_LIMIT, collective_id=1, has_side_effects=True),
        cost_estimate=pl.CostEstimate(flops=2 * n_exp * cap * d * inter, bytes_accessed=2 * n_exp * d * inter, transcendentals=0),
        name="down_reduce",
    )(slot_off, hidden, w_down, gate_col, base)


def solution(mesh):
    def local_block(hidden_in, norm_gain, router_w, w_gate, w_up, w_down, ws_gate, ws_up, ws_down, expert_ids):
        tok_dev, top_k = expert_ids.shape
        d = hidden_in.shape[1]
        n_exp = w_gate.shape[0]
        cap = 512
        sub = 4
        me = lax.axis_index("ep")
        x_norm = rms_norm(hidden_in, norm_gain)
        xn_all = lax.all_gather(x_norm, "ep", axis=0, tiled=True)
        gate_vals = route_gates(x_norm, router_w, expert_ids)
        ids_all = lax.all_gather(expert_ids, "ep", axis=0, tiled=True)
        gates_all = lax.all_gather(gate_vals, "ep", axis=0, tiled=True)
        shared_out = swiglu(x_norm, ws_gate, ws_up, ws_down)
        base = hidden_in.astype(jnp.float32) + shared_out.astype(jnp.float32)

        tokens = ids_all.shape[0]
        local = ids_all - me * n_exp
        hot = local[:, :, None] == jnp.arange(n_exp, dtype=jnp.int32)[None, None, :]
        hit = jnp.any(hot, axis=1)
        count = jnp.cumsum(hit.astype(jnp.int32), axis=0)
        slot = jnp.arange(n_exp, dtype=jnp.int32)[None, :] * cap + count - 1
        slot_off = jnp.sum(jnp.where(hot, slot[:, None, :], 0), axis=2)
        slot_off = jnp.where((local >= 0) & (local < n_exp), slot_off, n_exp * cap) * sub
        rank = jnp.arange(cap, dtype=jnp.int32)
        tok = jnp.sum((count.T[:, None, :] <= rank[None, :, None]).astype(jnp.int32), axis=2)
        tok_off = jnp.minimum(tok, tokens - 1).reshape(-1) * (d // LANES)
        gate_tok = jnp.sum(jnp.where(hot, gates_all[:, :, None], 0.0), axis=1)
        mine = (count.T[:, None, :] == rank[None, :, None] + 1) & hit.T[:, None, :]
        gate_col = jnp.sum(jnp.where(mine, gate_tok.T[:, None, :], 0.0), axis=2)[:, :, None]

        hidden = gate_up(tok_off, xn_all, w_gate, w_up)
        return down_reduce(slot_off.reshape(-1), hidden, w_down, gate_col, base)

    row_spec = P(("dp", "ep"), None)
    in_specs = (row_spec, P(), P(), P("ep"), P("ep"), P("ep"), P(), P(), P(), row_spec)
    return jax.shard_map(local_block, mesh=mesh, in_specs=in_specs, out_specs=row_spec, check_vma=False)
```

```python
import functools

import jax
import jax.numpy as jnp
from jax import lax
from jax.experimental import pallas as pl
from jax.experimental.pallas import tpu as pltpu
from jax.sharding import PartitionSpec as P

NORM_EPS = 1e-6
ROUTE_SCALE = 2.5
TOP = 6
WIDTHS = (768, 768, 768, 256)
SUB = 6
LANES = 128
MESH = pl.DeviceIdType.MESH
VMEM_LIMIT = 66_000_000


def neighbours():
    me = lax.axis_index("ep")
    core, bx, by = lax.rem(me, 2), lax.rem(me // 2, 2), me // 4
    return core, bx, by, me + 1 - 2 * core, me + 2 - 4 * bx, me + 4 - 8 * by


def gather_kernel(x_ref, gain_ref, rw_ref, ids_ref, wsg_hbm, wsu_hbm, wsd_hbm,
                  xn_all, base_ref, tok_ref, slot_ref, gcol_ref,
                  xn, wsg, wsu, wsd, hid, ids_all, gates_all, cnt, gtok, cnt3, gtok3,
                  w_sem, own_sem, meta_send, meta_recv, snd, rcv):
    tok_dev, d = x_ref.shape
    n_dev, top_pad = ids_all.shape[0], ids_all.shape[1]
    n_exp, tokens = cnt.shape
    cap = tok_ref.shape[2]
    half = tok_dev // 2
    ng, cg = wsg.shape[0], wsg.shape[2]
    nd, cd = wsd.shape[0], wsd.shape[2]
    core, bx, by, partner, xdev, ydev = neighbours()
    me = lax.axis_index("ep")
    diag = n_dev - 2 - (me - core) + core

    barrier = pltpu.get_barrier_semaphore()
    for j in range(1, n_dev):
        pl.semaphore_signal(barrier, inc=1, device_id={"ep": lax.rem(me + j, n_dev)}, device_id_type=MESH)

    def w_copies(c):
        at = pl.ds(pl.multiple_of(c * cg, LANES), cg)
        return [pltpu.make_async_copy(wsg_hbm.at[:, at], wsg.at[c], w_sem.at[0, c]), pltpu.make_async_copy(wsu_hbm.at[:, at], wsu.at[c], w_sem.at[1, c])]

    def d_copy(c):
        return pltpu.make_async_copy(wsd_hbm.at[:, pl.ds(pl.multiple_of(c * cd, LANES), cd)], wsd.at[c], w_sem.at[2, c])

    for c in range(ng):
        for cp in w_copies(c):
            cp.start()
    for c in range(nd):
        d_copy(c).start()

    def norm(b, _):
        at = pl.ds(pl.multiple_of(b * 16, 16), 16)
        x = x_ref[at, :].astype(jnp.float32)
        inv = lax.rsqrt(jnp.mean(x * x, axis=1, keepdims=True) + NORM_EPS)
        xn[at, :] = (x * inv * gain_ref[...]).astype(jnp.bfloat16)
        return 0
    lax.fori_loop(0, tok_dev // 16, norm, 0)

    pl.semaphore_wait(barrier, n_dev - 1)

    def remote(src, dst, k, dev):
        return pltpu.make_async_remote_copy(src_ref=src, dst_ref=dst, send_sem=snd.at[k], recv_sem=rcv.at[k], device_id={"ep": dev}, device_id_type=MESH)

    def rows(dev, h):
        return pl.ds(pl.multiple_of(dev * tok_dev + h * half, half), half)

    def mine(k, h, dev):
        return remote(xn.at[pl.ds(h * half, half)], xn_all.at[rows(me, h)], k, dev)

    def pass_on(k, src, h, dev):
        return remote(xn_all.at[rows(src, h)], xn_all.at[rows(src, h)], k, dev)

    own = pltpu.make_async_copy(xn, xn_all.at[pl.ds(pl.multiple_of(me * tok_dev, tok_dev), tok_dev)], own_sem)
    own.start()
    direct = [mine(0, 0, xdev), mine(1, 1, ydev), mine(2, 1, xdev), mine(3, 0, ydev), mine(4, 0, partner), mine(5, 1, partner)]
    for cp in direct:
        cp.start()

    def meta(j, which):
        ref = (ids_all, gates_all)[which]
        src = (ids_ref, gates_all.at[me])[which]
        dev = lax.rem(me + j, n_dev)
        return pltpu.make_async_remote_copy(src_ref=src, dst_ref=ref.at[me], send_sem=meta_send.at[which, j], recv_sem=meta_recv.at[which, j], device_id={"ep": dev}, device_id_type=MESH)

    for j in range(1, n_dev):
        meta(j, 0).start()
    ids_all[me] = ids_ref[...]

    logits = lax.dot_general(rw_ref[...], xn[...].astype(jnp.float32), (((1,), (1,)), ((), ())), precision=lax.Precision.HIGHEST, preferred_element_type=jnp.float32)
    scores = jax.nn.sigmoid(logits)
    names = lax.broadcasted_iota(jnp.int32, scores.shape, 0)
    picked = []
    for k in range(TOP):
        picked.append(jnp.sum(jnp.where(names == ids_ref[k:k + 1, :], scores, 0.0), axis=0, keepdims=True))
    total = picked[0]
    for k in range(1, TOP):
        total = total + picked[k]
    for k in range(TOP):
        gates_all[me, k:k + 1, :] = ROUTE_SCALE * picked[k] / total
    gates_all[me, TOP:top_pad, :] = jnp.zeros((top_pad - TOP, tok_dev), jnp.float32)
    for j in range(1, n_dev):
        meta(j, 1).start()

    def shared_up(c, _):
        for cp in w_copies(c):
            cp.wait()
        g = jnp.dot(xn[...], wsg[c], preferred_element_type=jnp.float32)
        u = jnp.dot(xn[...], wsu[c], preferred_element_type=jnp.float32)
        hid[:, pl.ds(pl.multiple_of(c * cg, LANES), cg)] = (g * jax.nn.sigmoid(g) * u).astype(jnp.bfloat16)
        return 0
    lax.fori_loop(0, ng, shared_up, 0)

    def shared_down(c, _):
        d_copy(c).wait()
        y = jnp.dot(hid[...], wsd[c], preferred_element_type=jnp.float32).astype(jnp.bfloat16)
        at = pl.ds(pl.multiple_of(c * cd, LANES), cd)
        base_ref[:, at] = x_ref[:, at].astype(jnp.float32) + y.astype(jnp.float32)
        return 0
    lax.fori_loop(0, nd, shared_down, 0)

    mine(0, 0, xdev).wait_recv()
    relay = [pass_on(6, xdev, 0, ydev)]
    relay[0].start()
    mine(1, 1, ydev).wait_recv()
    relay.append(pass_on(7, ydev, 1, xdev))
    relay[1].start()
    side = [pass_on(8, xdev, 0, partner), pass_on(9, ydev, 1, partner)]
    for cp in side:
        cp.start()

    for which in range(2):
        for j in range(1, n_dev):
            meta(j, which).wait_recv()

    def hits(dev, _):
        at = pl.ds(pl.multiple_of(dev * tok_dev, tok_dev), tok_dev)
        ids = ids_all[dev]
        gates = gates_all[dev]
        for e in range(n_exp):
            hot = ids == me * n_exp + e
            cnt[e:e + 1, at] = jnp.sum(jnp.where(hot, 1.0, 0.0), axis=0, keepdims=True)
            gtok[e:e + 1, at] = jnp.sum(jnp.where(hot, gates, 0.0), axis=0, keepdims=True)
        return 0
    lax.fori_loop(0, n_dev, hits, 0)

    upper = (lax.broadcasted_iota(jnp.int32, (LANES, LANES), 0) <= lax.broadcasted_iota(jnp.int32, (LANES, LANES), 1)).astype(jnp.float32).astype(jnp.bfloat16)
    run = jnp.zeros((n_exp, 1), jnp.float32)
    for i in range(tokens // LANES):
        at = slice(i * LANES, (i + 1) * LANES)
        hit = cnt[:, at]
        ranks = jnp.dot(hit.astype(jnp.bfloat16), upper, preferred_element_type=jnp.float32) + run
        run = ranks[:, LANES - 1:LANES]
        cnt[:, at] = ranks
        gate = jnp.where(hit > 0.0, gtok[:, at], 0.0)
        for e in range(n_exp):
            cnt3[e, :, at] = ranks[e:e + 1, :]
            gtok3[e, :, at] = gate[e:e + 1, :]

    def slots(dev, _):
        at = pl.ds(pl.multiple_of(dev * tok_dev, tok_dev), tok_dev)
        ids = ids_all[dev]
        slot = jnp.full(ids.shape, n_exp * cap, jnp.int32)
        for e in range(n_exp):
            slot = jnp.where(ids == me * n_exp + e, cnt[e:e + 1, at].astype(jnp.int32) + (e * cap - 1), slot)
        slot_ref[pl.ds(pl.multiple_of(dev * top_pad, top_pad), top_pad), :] = slot * SUB
        return 0
    lax.fori_loop(0, n_dev, slots, 0)

    mine(2, 1, xdev).wait_recv()
    mine(3, 0, ydev).wait_recv()
    more = [pass_on(10, xdev, 1, partner), pass_on(11, ydev, 0, partner)]
    for cp in more:
        cp.start()

    rb = 64
    eye = (lax.broadcasted_iota(jnp.int32, (LANES, LANES), 0) == lax.broadcasted_iota(jnp.int32, (LANES, LANES), 1))

    def table(e, _):
        for r0 in range(0, cap, LANES):
            cols = []
            for q in range(0, LANES, rb):
                rank = lax.broadcasted_iota(jnp.int32, (rb, LANES), 0).astype(jnp.float32) + float(r0 + q)
                before = jnp.zeros((rb, LANES), jnp.float32)
                gate = jnp.zeros((rb, LANES), jnp.float32)
                for i in range(tokens // LANES):
                    at = slice(i * LANES, (i + 1) * LANES)
                    c = cnt3[e, :, at]
                    before = before + jnp.where(c <= rank, 1.0, 0.0)
                    gate = gate + jnp.where(c == rank + 1.0, gtok3[e, :, at], 0.0)
                cols.append(jnp.sum(before, axis=1, keepdims=True))
                gcol_ref[e, r0 + q:r0 + q + rb, :] = jnp.broadcast_to(jnp.sum(gate, axis=1, keepdims=True), (rb, LANES))
            col = jnp.concatenate(cols, axis=0)
            row = jnp.sum(jnp.where(eye, col, 0.0), axis=0, keepdims=True)
            tok_ref[e, :, r0:r0 + LANES] = jnp.minimum(row, float(tokens - 1)).astype(jnp.int32) * (d // LANES)
        return 0
    lax.fori_loop(0, n_exp, table, 0)

    pass_on(6, diag, 0, ydev).wait_recv()
    last = [pass_on(12, diag, 0, partner)]
    last[0].start()
    pass_on(7, diag, 1, xdev).wait_recv()
    last.append(pass_on(13, diag, 1, partner))
    last[1].start()

    own.wait()
    for cp in direct + relay + side + more + last:
        cp.wait_send()
    for which in range(2):
        for j in range(1, n_dev):
            meta(j, which).wait_send()
    for k in (4, 5, 8, 9, 10, 11, 12, 13):
        mine(k, 0, partner).wait_recv()


def gather_rows(x, gain, router_w, ids_t, ws_gate, ws_up, ws_down, n_dev, n_exp, cap, cg=512, cd=512):
    tok_dev, d = x.shape
    inter = ws_gate.shape[1]
    tokens, top_pad = n_dev * tok_dev, ids_t.shape[0]
    f32, i32, bf16 = jnp.float32, jnp.int32, jnp.bfloat16
    vmem = pl.BlockSpec(memory_space=pltpu.VMEM)
    hbm = pl.BlockSpec(memory_space=pl.ANY)
    return pl.pallas_call(
        gather_kernel,
        out_shape=(
            jax.ShapeDtypeStruct((tokens, d), bf16),
            jax.ShapeDtypeStruct((tok_dev, d), f32),
            jax.ShapeDtypeStruct((n_exp, 1, cap), i32),
            jax.ShapeDtypeStruct((n_dev * top_pad, tok_dev), i32),
            jax.ShapeDtypeStruct((n_exp, cap, LANES), f32),
        ),
        in_specs=[vmem, vmem, vmem, vmem, hbm, hbm, hbm],
        out_specs=(hbm, vmem, vmem, vmem, vmem),
        scratch_shapes=[
            pltpu.VMEM((tok_dev, d), bf16),
            pltpu.VMEM((inter // cg, d, cg), bf16),
            pltpu.VMEM((inter // cg, d, cg), bf16),
            pltpu.VMEM((d // cd, inter, cd), bf16),
            pltpu.VMEM((tok_dev, inter), bf16),
            pltpu.VMEM((n_dev, top_pad, tok_dev), i32),
            pltpu.VMEM((n_dev, top_pad, tok_dev), f32),
            pltpu.VMEM((n_exp, tokens), f32),
            pltpu.VMEM((n_exp, tokens), f32),
            pltpu.VMEM((n_exp, 1, tokens), f32),
            pltpu.VMEM((n_exp, 1, tokens), f32),
            pltpu.SemaphoreType.DMA((3, max(inter // cg, d // cd))),
            pltpu.SemaphoreType.DMA,
            pltpu.SemaphoreType.DMA((2, n_dev)),
            pltpu.SemaphoreType.DMA((2, n_dev)),
            pltpu.SemaphoreType.DMA((14,)),
            pltpu.SemaphoreType.DMA((14,)),
        ],
        compiler_params=pltpu.CompilerParams(vmem_limit_bytes=VMEM_LIMIT, collective_id=2, has_side_effects=True),
        cost_estimate=pl.CostEstimate(flops=6 * tok_dev * d * inter, bytes_accessed=6 * d * inter, transcendentals=0),
        name="gather_rows",
    )(x, gain, router_w, ids_t, ws_gate, ws_up, ws_down)


def gate_up_kernel(tok_ref, xn_ref, wg_ref, wu_ref, h_ref, xf, gbuf, lhs):
    e = pl.program_id(0)
    j = pl.program_id(1)
    cap, d = lhs.shape
    nc = d // LANES

    @pl.when((e == 0) & (j == 0))
    def _():
        def widen(b, _):
            rows = pl.multiple_of(b * 64, 64)
            blk = xn_ref[pl.ds(rows, 64), :].astype(jnp.float32)
            for c in range(nc):
                xf[pl.ds(rows * nc + c, 64, stride=nc), :] = blk[:, c * LANES:(c + 1) * LANES]
            return 0
        lax.fori_loop(0, xn_ref.shape[0] // 64, widen, 0)

    @pl.when(j == 0)
    def _():
        def gather(b, _):
            for u in range(16):
                r = b * 16 + u
                gbuf[pl.ds(r * nc, nc), :] = xf[pl.ds(tok_ref[e * cap + r], nc), :]
            return 0
        lax.fori_loop(0, cap // 16, gather, 0)

        def narrow(b, _):
            rows = pl.multiple_of(b * 64, 64)
            for c in range(nc):
                lhs[pl.ds(rows, 64), c * LANES:(c + 1) * LANES] = gbuf[pl.ds(rows * nc + c, 64, stride=nc), :].astype(jnp.bfloat16)
            return 0
        lax.fori_loop(0, cap // 64, narrow, 0)

    g = jnp.dot(lhs[...], wg_ref[0], preferred_element_type=jnp.float32)
    u = jnp.dot(lhs[...], wu_ref[0], preferred_element_type=jnp.float32)
    h_ref[0] = (g * jax.nn.sigmoid(g) * u).astype(jnp.bfloat16)


def gate_up(tok_off, xn_all, w_gate, w_up, block=512):
    n_exp, d, inter = w_gate.shape
    cap = tok_off.shape[0] // n_exp
    tokens = xn_all.shape[0]
    return pl.pallas_call(
        gate_up_kernel,
        grid_spec=pltpu.PrefetchScalarGridSpec(
            num_scalar_prefetch=1,
            grid=(n_exp, inter // block),
            in_specs=[
                pl.BlockSpec((tokens, d), lambda e, j, t: (0, 0), pipeline_mode=pl.Buffered(1)),
                pl.BlockSpec((1, d, block), lambda e, j, t: (e, 0, j)),
                pl.BlockSpec((1, d, block), lambda e, j, t: (e, 0, j)),
            ],
            out_specs=pl.BlockSpec((1, cap, block), lambda e, j, t: (e, 0, j)),
            scratch_shapes=[
                pltpu.VMEM((tokens * d // LANES, LANES), jnp.float32),
                pltpu.VMEM((cap * d // LANES, LANES), jnp.float32),
                pltpu.VMEM((cap, d), jnp.bfloat16),
            ],
        ),
        out_shape=jax.ShapeDtypeStruct((n_exp, cap, inter), jnp.bfloat16),
        compiler_params=pltpu.CompilerParams(vmem_limit_bytes=VMEM_LIMIT, dimension_semantics=("arbitrary", "arbitrary")),
        cost_estimate=pl.CostEstimate(flops=4 * n_exp * cap * d * inter, bytes_accessed=4 * n_exp * d * inter, transcendentals=0),
        name="gate_up",
    )(tok_off, xn_all, w_gate, w_up)


def down_kernel(slot_ref, h_hbm, wd_hbm, gate_ref, out_ref,
                h, wd, ybuf, part, sums, got_x, got_y, got_2,
                h_sem, wd_sem, send_core, recv_core, send_x, recv_x, send_y, recv_y, send_2, recv_2):
    n_exp, cap, inter = h.shape
    tok_dev = out_ref.shape[0]
    half = tok_dev // 2
    core, bx, by, partner, xdev, ydev = neighbours()
    chip_d, chip_x, chip_y, chip_o = 2 * (1 - by) + 1 - bx, 2 * by + 1 - bx, 2 * (1 - by) + bx, 2 * by + bx
    chips = (chip_d, chip_x, chip_y, chip_o)
    subs = [w // LANES for w in WIDTHS]
    offs = [sum(subs[:c]) for c in range(len(subs))]

    barrier = pltpu.get_barrier_semaphore()
    for dev in (partner, xdev, ydev):
        pl.semaphore_signal(barrier, inc=1, device_id={"ep": dev}, device_id_type=MESH)

    def h_copy(e):
        return pltpu.make_async_copy(h_hbm.at[e], h.at[e], h_sem.at[e])

    def wd_copy(c, e):
        slot = lax.rem(c * n_exp + e, 3)
        return pltpu.make_async_copy(wd_hbm.at[e, :, pl.ds(offs[c] * LANES, WIDTHS[c])], wd.at[slot, :, pl.ds(0, WIDTHS[c])], wd_sem.at[slot])

    h_copy(0).start()
    wd_copy(0, 0).start()
    wd_copy(0, 1).start()
    for e in range(1, n_exp):
        h_copy(e).start()
    ybuf[pl.ds(n_exp * cap * SUB, 8), :] = jnp.zeros((8, LANES), jnp.float32)
    pl.semaphore_wait(barrier, 3)

    def remote(src, dst, send, recv, dev):
        return pltpu.make_async_remote_copy(src_ref=src, dst_ref=dst, send_sem=send, recv_sem=recv, device_id={"ep": dev}, device_id_type=MESH)

    def full(c):
        return pl.ds(offs[c] * tok_dev, subs[c] * tok_dev)

    def low(c):
        return pl.ds(offs[c] * tok_dev, subs[c] * half)

    def high(c):
        return pl.ds(offs[c] * tok_dev + subs[c] * half, subs[c] * half)

    def land(c):
        return pl.ds(offs[c] * half, subs[c] * half)

    def core_copy(c, i):
        return remote(part.at[2 * chips[i] + 1 - core, pl.ds(0, subs[c] * tok_dev)], sums.at[chips[i], full(c)], send_core.at[c, i], recv_core.at[c, i], partner)

    def x_copy(c, i):
        return remote(sums.at[(chip_d, chip_x)[i], low(c)], got_x.at[i, land(c)], send_x.at[c, i], recv_x.at[c, i], xdev)

    def y_copy(c, i):
        return remote(sums.at[(chip_d, chip_y)[i], high(c)], got_y.at[i, land(c)], send_y.at[c, i], recv_y.at[c, i], ydev)

    def hop_copy(c, i):
        if i == 0:
            return remote(sums.at[chip_y, low(c)], got_2.at[0, land(c)], send_2.at[c, 0], recv_2.at[c, 0], ydev)
        return remote(sums.at[chip_x, high(c)], got_2.at[1, land(c)], send_2.at[c, 1], recv_2.at[c, 1], xdev)

    def add_into(dst, src, n):
        def one(i, _):
            at = pl.ds(pl.multiple_of(i * 128, 128), 128)
            dst[at, :] = dst[at, :] + src[at, :]
            return 0
        lax.fori_loop(0, n // 128, one, 0)

    def on_core(c, i):
        core_copy(c, i).wait_recv()
        add_into(sums.at[chips[i], full(c)], part.at[2 * chips[i] + core, pl.ds(0, subs[c] * tok_dev)], subs[c] * tok_dev)
        if i == 0:
            x_copy(c, 0).start()
            y_copy(c, 0).start()
        elif i == 1:
            x_copy(c, 1).start()
        elif i == 2:
            y_copy(c, 1).start()

    def on_first(c):
        x_copy(c, 0).wait_recv()
        add_into(sums.at[chip_y, low(c)], got_x.at[0, land(c)], subs[c] * half)
        hop_copy(c, 0).start()
        y_copy(c, 0).wait_recv()
        add_into(sums.at[chip_x, high(c)], got_y.at[0, land(c)], subs[c] * half)
        hop_copy(c, 1).start()

    def on_own(c):
        x_copy(c, 1).wait_recv()
        add_into(sums.at[chip_o, low(c)], got_x.at[1, land(c)], subs[c] * half)
        y_copy(c, 1).wait_recv()
        add_into(sums.at[chip_o, high(c)], got_y.at[1, land(c)], subs[c] * half)

    def finish(c):
        hop_copy(c, 0).wait_recv()
        add_into(sums.at[chip_o, low(c)], got_2.at[0, land(c)], subs[c] * half)
        hop_copy(c, 1).wait_recv()
        add_into(sums.at[chip_o, high(c)], got_2.at[1, land(c)], subs[c] * half)
        for i in range(subs[c]):
            at = (offs[c] + i) * LANES
            out_ref[:, at:at + LANES] = sums[chip_o, pl.ds(offs[c] * tok_dev + i, tok_dev, stride=subs[c]), :]

    def down(c, lo, hi):
        width = WIDTHS[c]

        def one(e, _):
            slot = lax.rem(c * n_exp + e, 3)
            @pl.when(e + 2 < n_exp)
            def _():
                wd_copy(c, e + 2).start()
            if c + 1 < len(WIDTHS):
                @pl.when(e + 2 >= n_exp)
                def _():
                    wd_copy(c + 1, e + 2 - n_exp).start()
            if c == 0:
                h_copy(e).wait()
            wd_copy(c, e).wait()
            y = jnp.dot(h[e], wd[slot, :, 0:width], preferred_element_type=jnp.float32)
            y = y.astype(jnp.bfloat16).astype(jnp.float32)
            gate = gate_ref[e]
            for i in range(subs[c]):
                ybuf[pl.ds(e * (cap * SUB) + i, cap, stride=SUB), :] = y[:, i * LANES:(i + 1) * LANES] * gate
            return 0
        lax.fori_loop(lo, hi, one, 0)

    def combine(c, i):
        sub = subs[c]

        def one_dev(j, _):
            dev = 2 * chips[i] + j

            def one(b, _):
                at = dev * (8 * tok_dev) + b * 8
                for u in range(8):
                    acc = ybuf[pl.ds(slot_ref[at + u], sub), :]
                    for k in range(1, TOP):
                        acc = acc + ybuf[pl.ds(slot_ref[at + (k * tok_dev + u)], sub), :]
                    part[dev, pl.ds(b * (8 * sub) + u * sub, sub), :] = acc
                return 0
            lax.fori_loop(0, tok_dev // 8, one, 0)
            return 0
        lax.fori_loop(0, 2, one_dev, 0)

    last = len(WIDTHS) - 1
    for c in range(len(WIDTHS)):
        down(c, 0, 1)
        if c >= 1:
            on_core(c - 1, 3)
        down(c, 1, n_exp // 2)
        if c >= 1:
            on_first(c - 1)
        down(c, n_exp // 2, n_exp)
        if c >= 2:
            on_own(c - 2)
            finish(c - 2)
        for i in range(4):
            if c >= 1:
                core_copy(c - 1, i).wait_send()
            combine(c, i)
            core_copy(c, i).start()
            if i >= 1:
                on_core(c, i - 1)
    on_core(last, 3)
    on_first(last)
    on_own(last - 1)
    finish(last - 1)
    on_own(last)
    finish(last)
    for c in range(len(WIDTHS)):
        for i in range(2):
            x_copy(c, i).wait_send()
            y_copy(c, i).wait_send()
            hop_copy(c, i).wait_send()
    for i in range(4):
        core_copy(last, i).wait_send()


def down_reduce(slot_off, hidden, w_down, gate_col, tok_dev):
    n_exp, cap, inter = hidden.shape
    d = w_down.shape[2]
    n_chunk = len(WIDTHS)
    rows = tok_dev * d // LANES
    f32 = jnp.float32
    return pl.pallas_call(
        down_kernel,
        out_shape=jax.ShapeDtypeStruct((tok_dev, d), f32),
        in_specs=[
            pl.BlockSpec(memory_space=pltpu.SMEM),
            pl.BlockSpec(memory_space=pl.ANY),
            pl.BlockSpec(memory_space=pl.ANY),
            pl.BlockSpec(memory_space=pltpu.VMEM),
        ],
        out_specs=pl.BlockSpec(memory_space=pltpu.VMEM),
        scratch_shapes=[
            pltpu.VMEM((n_exp, cap, inter), jnp.bfloat16),
            pltpu.VMEM((3, inter, max(WIDTHS)), jnp.bfloat16),
            pltpu.VMEM((n_exp * cap * SUB + 8, LANES), f32),
            pltpu.VMEM((8, tok_dev * SUB, LANES), f32),
            pltpu.VMEM((4, rows, LANES), f32),
            pltpu.VMEM((2, rows // 2, LANES), f32),
            pltpu.VMEM((2, rows // 2, LANES), f32),
            pltpu.VMEM((2, rows // 2, LANES), f32),
            pltpu.SemaphoreType.DMA((n_exp,)),
            pltpu.SemaphoreType.DMA((3,)),
            pltpu.SemaphoreType.DMA((n_chunk, 4)),
            pltpu.SemaphoreType.DMA((n_chunk, 4)),
            pltpu.SemaphoreType.DMA((n_chunk, 2)),
            pltpu.SemaphoreType.DMA((n_chunk, 2)),
            pltpu.SemaphoreType.DMA((n_chunk, 2)),
            pltpu.SemaphoreType.DMA((n_chunk, 2)),
            pltpu.SemaphoreType.DMA((n_chunk, 2)),
            pltpu.SemaphoreType.DMA((n_chunk, 2)),
        ],
        compiler_params=pltpu.CompilerParams(vmem_limit_bytes=VMEM_LIMIT, collective_id=1, has_side_effects=True),
        cost_estimate=pl.CostEstimate(flops=2 * n_exp * cap * d * inter, bytes_accessed=2 * n_exp * d * inter, transcendentals=0),
        name="down_reduce",
    )(slot_off, hidden, w_down, gate_col)


def solution(mesh):
    n_dev = mesh.shape["ep"]

    def local_block(hidden_in, norm_gain, router_w, w_gate, w_up, w_down, ws_gate, ws_up, ws_down, expert_ids):
        n_exp = w_gate.shape[0]
        cap = 512
        ids_t = jnp.pad(expert_ids.T, ((0, 8 - TOP), (0, 0)), constant_values=-1)
        xn_all, base, tok_off, slots, gate_col = gather_rows(hidden_in, norm_gain[None, :], router_w, ids_t, ws_gate, ws_up, ws_down, n_dev, n_exp, cap)
        hidden = gate_up(tok_off.reshape(-1), xn_all, w_gate, w_up)
        routed = down_reduce(slots.reshape(-1), hidden, w_down, gate_col, hidden_in.shape[0])
        return (base + routed).astype(jnp.bfloat16)

    row_spec = P(("dp", "ep"), None)
    in_specs = (row_spec, P(), P(), P("ep"), P("ep"), P("ep"), P(), P(), P(), row_spec)
    return jax.shard_map(local_block, mesh=mesh, in_specs=in_specs, out_specs=row_spec, check_vma=False)
```

```python
import functools

import jax
import jax.numpy as jnp
from jax import lax
from jax.experimental import pallas as pl
from jax.experimental.pallas import tpu as pltpu
from jax.sharding import PartitionSpec as P

NORM_EPS = 1e-6
ROUTE_SCALE = 2.5
TOP = 6
WIDTHS = (768, 768, 768, 256)
SUB = 6
LANES = 128
MESH = pl.DeviceIdType.MESH
VMEM_LIMIT = 66_000_000


def neighbours():
    me = lax.axis_index("ep")
    core, bx, by = lax.rem(me, 2), lax.rem(me // 2, 2), me // 4
    return core, bx, by, me + 1 - 2 * core, me + 2 - 4 * bx, me + 4 - 8 * by


def gather_kernel(x_ref, gain_ref, rw_ref, ids_ref, wsg_hbm, wsu_hbm, wsd_hbm,
                  xn_all, base_hbm, tok_ref, slot_ref, gcol_hbm,
                  base_ref, gcol_ref, xn, wsg, wsu, wsd, hid, ids_all, gates_all, cnt, gtok, cnt3, gtok3,
                  w_sem, own_sem, out_sem, meta_send, meta_recv, snd, rcv):
    tok_dev, d = x_ref.shape
    n_dev, top_pad = ids_all.shape[0], ids_all.shape[1]
    n_exp, tokens = cnt.shape
    cap = tok_ref.shape[2]
    half = tok_dev // 2
    ng, cg = wsg.shape[0], wsg.shape[2]
    nd, cd = wsd.shape[0], wsd.shape[2]
    core, bx, by, partner, xdev, ydev = neighbours()
    me = lax.axis_index("ep")
    diag = n_dev - 2 - (me - core) + core

    barrier = pltpu.get_barrier_semaphore()
    for j in range(1, n_dev):
        pl.semaphore_signal(barrier, inc=1, device_id={"ep": lax.rem(me + j, n_dev)}, device_id_type=MESH)

    def w_copies(c):
        at = pl.ds(pl.multiple_of(c * cg, LANES), cg)
        return [pltpu.make_async_copy(wsg_hbm.at[:, at], wsg.at[c], w_sem.at[0, c]), pltpu.make_async_copy(wsu_hbm.at[:, at], wsu.at[c], w_sem.at[1, c])]

    def d_copy(c):
        return pltpu.make_async_copy(wsd_hbm.at[:, pl.ds(pl.multiple_of(c * cd, LANES), cd)], wsd.at[c], w_sem.at[2, c])

    for c in range(ng):
        for cp in w_copies(c):
            cp.start()
    for c in range(nd):
        d_copy(c).start()

    def norm(b, _):
        at = pl.ds(pl.multiple_of(b * 32, 32), 32)
        x = x_ref[at, :].astype(jnp.float32)
        inv = lax.rsqrt(jnp.mean(x * x, axis=1, keepdims=True) + NORM_EPS)
        xn[at, :] = (x * inv * gain_ref[...]).astype(jnp.bfloat16)
        return 0
    lax.fori_loop(0, tok_dev // 32, norm, 0)

    pl.semaphore_wait(barrier, n_dev - 1)

    def remote(src, dst, k, dev):
        return pltpu.make_async_remote_copy(src_ref=src, dst_ref=dst, send_sem=snd.at[k], recv_sem=rcv.at[k], device_id={"ep": dev}, device_id_type=MESH)

    def rows(dev, h):
        return pl.ds(pl.multiple_of(dev * tok_dev + h * half, half), half)

    def mine(k, h, dev):
        return remote(xn.at[pl.ds(h * half, half)], xn_all.at[rows(me, h)], k, dev)

    def pass_on(k, src, h, dev):
        return remote(xn_all.at[rows(src, h)], xn_all.at[rows(src, h)], k, dev)

    own = pltpu.make_async_copy(xn, xn_all.at[pl.ds(pl.multiple_of(me * tok_dev, tok_dev), tok_dev)], own_sem)
    own.start()
    direct = [mine(0, 0, xdev), mine(1, 1, ydev), mine(2, 1, xdev), mine(3, 0, ydev), mine(4, 0, partner), mine(5, 1, partner)]
    for cp in direct:
        cp.start()

    def meta(j, which):
        ref = (ids_all, gates_all)[which]
        src = (ids_ref, gates_all.at[me])[which]
        dev = lax.rem(me + j, n_dev)
        return pltpu.make_async_remote_copy(src_ref=src, dst_ref=ref.at[me], send_sem=meta_send.at[which, j], recv_sem=meta_recv.at[which, j], device_id={"ep": dev}, device_id_type=MESH)

    for j in range(1, n_dev):
        meta(j, 0).start()
    ids_all[me] = ids_ref[...]

    logits = lax.dot_general(rw_ref[...], xn[...].astype(jnp.float32), (((1,), (1,)), ((), ())), precision=lax.Precision.HIGHEST, preferred_element_type=jnp.float32)
    scores = jax.nn.sigmoid(logits)
    names = lax.broadcasted_iota(jnp.int32, scores.shape, 0)
    picked = []
    for k in range(TOP):
        picked.append(jnp.sum(jnp.where(names == ids_ref[k:k + 1, :], scores, 0.0), axis=0, keepdims=True))
    total = picked[0]
    for k in range(1, TOP):
        total = total + picked[k]
    for k in range(TOP):
        gates_all[me, k:k + 1, :] = ROUTE_SCALE * picked[k] / total
    gates_all[me, TOP:top_pad, :] = jnp.zeros((top_pad - TOP, tok_dev), jnp.float32)
    for j in range(1, n_dev):
        meta(j, 1).start()

    def shared_up(c, _):
        for cp in w_copies(c):
            cp.wait()
        g = jnp.dot(xn[...], wsg[c], preferred_element_type=jnp.float32)
        u = jnp.dot(xn[...], wsu[c], preferred_element_type=jnp.float32)
        hid[:, pl.ds(pl.multiple_of(c * cg, LANES), cg)] = (g * jax.nn.sigmoid(g) * u).astype(jnp.bfloat16)
        return 0
    lax.fori_loop(0, ng, shared_up, 0)

    def shared_down(c, _):
        d_copy(c).wait()
        y = jnp.dot(hid[...], wsd[c], preferred_element_type=jnp.float32).astype(jnp.bfloat16)
        at = pl.ds(pl.multiple_of(c * cd, LANES), cd)
        base_ref[:, at] = x_ref[:, at].astype(jnp.float32) + y.astype(jnp.float32)
        return 0
    lax.fori_loop(0, nd, shared_down, 0)
    base_out = pltpu.make_async_copy(base_ref, base_hbm, out_sem.at[0])
    base_out.start()

    mine(0, 0, xdev).wait_recv()
    relay = [pass_on(6, xdev, 0, ydev)]
    relay[0].start()
    mine(1, 1, ydev).wait_recv()
    relay.append(pass_on(7, ydev, 1, xdev))
    relay[1].start()
    side = [pass_on(8, xdev, 0, partner), pass_on(9, ydev, 1, partner)]
    for cp in side:
        cp.start()

    for which in range(2):
        for j in range(1, n_dev):
            meta(j, which).wait_recv()

    def hits(dev, _):
        at = pl.ds(pl.multiple_of(dev * tok_dev, tok_dev), tok_dev)
        ids = ids_all[dev]
        gates = gates_all[dev]
        for e in range(n_exp):
            hot = ids == me * n_exp + e
            cnt[e:e + 1, at] = jnp.sum(jnp.where(hot, 1.0, 0.0), axis=0, keepdims=True)
            gtok[e:e + 1, at] = jnp.sum(jnp.where(hot, gates, 0.0), axis=0, keepdims=True)
        return 0
    lax.fori_loop(0, n_dev, hits, 0)

    upper = (lax.broadcasted_iota(jnp.int32, (LANES, LANES), 0) <= lax.broadcasted_iota(jnp.int32, (LANES, LANES), 1)).astype(jnp.float32).astype(jnp.bfloat16)
    run = jnp.zeros((n_exp, 1), jnp.float32)
    for i in range(tokens // LANES):
        at = slice(i * LANES, (i + 1) * LANES)
        hit = cnt[:, at]
        ranks = jnp.dot(hit.astype(jnp.bfloat16), upper, preferred_element_type=jnp.float32) + run
        run = ranks[:, LANES - 1:LANES]
        cnt[:, at] = ranks
        gate = jnp.where(hit > 0.0, gtok[:, at], 0.0)
        for e in range(n_exp):
            cnt3[e, :, at] = ranks[e:e + 1, :]
            gtok3[e, :, at] = gate[e:e + 1, :]

    def slots(dev, _):
        at = pl.ds(pl.multiple_of(dev * tok_dev, tok_dev), tok_dev)
        ids = ids_all[dev]
        slot = jnp.full(ids.shape, n_exp * cap, jnp.int32)
        for e in range(n_exp):
            slot = jnp.where(ids == me * n_exp + e, cnt[e:e + 1, at].astype(jnp.int32) + (e * cap - 1), slot)
        slot_ref[pl.ds(pl.multiple_of(dev * top_pad, top_pad), top_pad), :] = slot * SUB
        return 0
    lax.fori_loop(0, n_dev, slots, 0)

    mine(2, 1, xdev).wait_recv()
    mine(3, 0, ydev).wait_recv()
    more = [pass_on(10, xdev, 1, partner), pass_on(11, ydev, 0, partner)]
    for cp in more:
        cp.start()

    rb = 64
    eye = (lax.broadcasted_iota(jnp.int32, (LANES, LANES), 0) == lax.broadcasted_iota(jnp.int32, (LANES, LANES), 1))

    def table(e, _):
        for r0 in range(0, cap, LANES):
            cols = []
            for q in range(0, LANES, rb):
                rank = lax.broadcasted_iota(jnp.int32, (rb, LANES), 0).astype(jnp.float32) + float(r0 + q)
                before = jnp.zeros((rb, LANES), jnp.float32)
                gate = jnp.zeros((rb, LANES), jnp.float32)
                for i in range(tokens // LANES):
                    at = slice(i * LANES, (i + 1) * LANES)
                    c = cnt3[e, :, at]
                    before = before + jnp.where(c <= rank, 1.0, 0.0)
                    gate = gate + jnp.where(c == rank + 1.0, gtok3[e, :, at], 0.0)
                cols.append(jnp.sum(before, axis=1, keepdims=True))
                gcol_ref[e, r0 + q:r0 + q + rb, :] = jnp.broadcast_to(jnp.sum(gate, axis=1, keepdims=True), (rb, LANES))
            col = jnp.concatenate(cols, axis=0)
            row = jnp.sum(jnp.where(eye, col, 0.0), axis=0, keepdims=True)
            tok_ref[e, :, r0:r0 + LANES] = jnp.minimum(row, float(tokens - 1)).astype(jnp.int32) * (d // LANES)
        return 0
    lax.fori_loop(0, n_exp, table, 0)
    gcol_out = pltpu.make_async_copy(gcol_ref, gcol_hbm, out_sem.at[1])
    gcol_out.start()

    pass_on(6, diag, 0, ydev).wait_recv()
    last = [pass_on(12, diag, 0, partner)]
    last[0].start()
    pass_on(7, diag, 1, xdev).wait_recv()
    last.append(pass_on(13, diag, 1, partner))
    last[1].start()

    own.wait()
    base_out.wait()
    gcol_out.wait()
    for cp in direct + relay + side + more + last:
        cp.wait_send()
    for which in range(2):
        for j in range(1, n_dev):
            meta(j, which).wait_send()
    for k in (4, 5, 8, 9, 10, 11, 12, 13):
        mine(k, 0, partner).wait_recv()


def gather_rows(x, gain, router_w, ids_t, ws_gate, ws_up, ws_down, n_dev, n_exp, cap, cg=512, cd=512):
    tok_dev, d = x.shape
    inter = ws_gate.shape[1]
    tokens, top_pad = n_dev * tok_dev, ids_t.shape[0]
    f32, i32, bf16 = jnp.float32, jnp.int32, jnp.bfloat16
    vmem = pl.BlockSpec(memory_space=pltpu.VMEM)
    hbm = pl.BlockSpec(memory_space=pl.ANY)
    return pl.pallas_call(
        gather_kernel,
        out_shape=(
            jax.ShapeDtypeStruct((tokens, d), bf16),
            jax.ShapeDtypeStruct((tok_dev, d), f32),
            jax.ShapeDtypeStruct((n_exp, 1, cap), i32),
            jax.ShapeDtypeStruct((n_dev * top_pad, tok_dev), i32),
            jax.ShapeDtypeStruct((n_exp, cap, LANES), f32),
        ),
        in_specs=[vmem, vmem, vmem, vmem, hbm, hbm, hbm],
        out_specs=(hbm, hbm, vmem, vmem, hbm),
        scratch_shapes=[
            pltpu.VMEM((tok_dev, d), f32),
            pltpu.VMEM((n_exp, cap, LANES), f32),
            pltpu.VMEM((tok_dev, d), bf16),
            pltpu.VMEM((inter // cg, d, cg), bf16),
            pltpu.VMEM((inter // cg, d, cg), bf16),
            pltpu.VMEM((d // cd, inter, cd), bf16),
            pltpu.VMEM((tok_dev, inter), bf16),
            pltpu.VMEM((n_dev, top_pad, tok_dev), i32),
            pltpu.VMEM((n_dev, top_pad, tok_dev), f32),
            pltpu.VMEM((n_exp, tokens), f32),
            pltpu.VMEM((n_exp, tokens), f32),
            pltpu.VMEM((n_exp, 1, tokens), f32),
            pltpu.VMEM((n_exp, 1, tokens), f32),
            pltpu.SemaphoreType.DMA((3, max(inter // cg, d // cd))),
            pltpu.SemaphoreType.DMA,
            pltpu.SemaphoreType.DMA((2,)),
            pltpu.SemaphoreType.DMA((2, n_dev)),
            pltpu.SemaphoreType.DMA((2, n_dev)),
            pltpu.SemaphoreType.DMA((14,)),
            pltpu.SemaphoreType.DMA((14,)),
        ],
        compiler_params=pltpu.CompilerParams(vmem_limit_bytes=VMEM_LIMIT, collective_id=2, has_side_effects=True),
        cost_estimate=pl.CostEstimate(flops=6 * tok_dev * d * inter, bytes_accessed=6 * d * inter, transcendentals=0),
        name="gather_rows",
    )(x, gain, router_w, ids_t, ws_gate, ws_up, ws_down)


def gate_up_kernel(tok_ref, xn_ref, wg_ref, wu_ref, h_ref, xf, gbuf, lhs_a, lhs_b):
    e = pl.program_id(0)
    j = pl.program_id(1)
    n_exp = pl.num_programs(0)
    cap, d = lhs_a.shape
    nc = d // LANES
    piece = gbuf.shape[0] // nc

    def gather(ex, r0):
        at = ex * cap + r0
        for u in range(piece):
            gbuf[pl.ds(u * nc, nc), :] = xf[pl.ds(tok_ref[at + u], nc), :]

    def narrow(dst, r0):
        for c in range(nc):
            dst[pl.ds(r0, piece), c * LANES:(c + 1) * LANES] = gbuf[pl.ds(c, piece, stride=nc), :].astype(jnp.bfloat16)

    @pl.when((e == 0) & (j == 0))
    def _():
        def widen(b, _):
            rows = pl.multiple_of(b * 64, 64)
            blk = xn_ref[pl.ds(rows, 64), :].astype(jnp.float32)
            for c in range(nc):
                xf[pl.ds(rows * nc + c, 64, stride=nc), :] = blk[:, c * LANES:(c + 1) * LANES]
            return 0
        lax.fori_loop(0, xn_ref.shape[0] // 64, widen, 0)

        def first(i, _):
            r0 = pl.multiple_of(jnp.minimum(i * piece, cap - piece), 16)
            gather(0, r0)
            narrow(lhs_a, r0)
            return 0
        lax.fori_loop(0, pl.cdiv(cap, piece), first, 0)

    def step(cur, nxt):
        r0 = pl.multiple_of(jnp.minimum(j * piece, cap - piece), 16)
        gather(jnp.minimum(e + 1, n_exp - 1), r0)
        g = jnp.dot(cur[...], wg_ref[0], preferred_element_type=jnp.float32)
        narrow(nxt, r0)
        u = jnp.dot(cur[...], wu_ref[0], preferred_element_type=jnp.float32)
        h_ref[0] = (g * jax.nn.sigmoid(g) * u).astype(jnp.bfloat16)

    @pl.when(lax.rem(e, 2) == 0)
    def _():
        step(lhs_a, lhs_b)

    @pl.when(lax.rem(e, 2) == 1)
    def _():
        step(lhs_b, lhs_a)


def gate_up(tok_off, xn_all, w_gate, w_up, block=512):
    n_exp, d, inter = w_gate.shape
    cap = tok_off.shape[0] // n_exp
    tokens = xn_all.shape[0]
    steps = inter // block
    piece = -(-cap // (16 * steps)) * 16
    return pl.pallas_call(
        gate_up_kernel,
        grid_spec=pltpu.PrefetchScalarGridSpec(
            num_scalar_prefetch=1,
            grid=(n_exp, inter // block),
            in_specs=[
                pl.BlockSpec((tokens, d), lambda e, j, t: (0, 0), pipeline_mode=pl.Buffered(1)),
                pl.BlockSpec((1, d, block), lambda e, j, t: (e, 0, j)),
                pl.BlockSpec((1, d, block), lambda e, j, t: (e, 0, j)),
            ],
            out_specs=pl.BlockSpec((1, cap, block), lambda e, j, t: (e, 0, j)),
            scratch_shapes=[
                pltpu.VMEM((tokens * d // LANES, LANES), jnp.float32),
                pltpu.VMEM((piece * d // LANES, LANES), jnp.float32),
                pltpu.VMEM((cap, d), jnp.bfloat16),
                pltpu.VMEM((cap, d), jnp.bfloat16),
            ],
        ),
        out_shape=jax.ShapeDtypeStruct((n_exp, cap, inter), jnp.bfloat16),
        compiler_params=pltpu.CompilerParams(vmem_limit_bytes=VMEM_LIMIT, dimension_semantics=("arbitrary", "arbitrary")),
        cost_estimate=pl.CostEstimate(flops=4 * n_exp * cap * d * inter, bytes_accessed=4 * n_exp * d * inter, transcendentals=0),
        name="gate_up",
    )(tok_off, xn_all, w_gate, w_up)


def down_kernel(slot_ref, h_hbm, wd_hbm, gate_ref, out_ref,
                h, wd, ybuf, part, sums, got_x, got_y, got_2,
                h_sem, wd_sem, send_core, recv_core, send_x, recv_x, send_y, recv_y, send_2, recv_2):
    n_exp, cap, inter = h.shape
    tok_dev = out_ref.shape[0]
    half = tok_dev // 2
    core, bx, by, partner, xdev, ydev = neighbours()
    chip_d, chip_x, chip_y, chip_o = 2 * (1 - by) + 1 - bx, 2 * by + 1 - bx, 2 * (1 - by) + bx, 2 * by + bx
    chips = (chip_d, chip_x, chip_y, chip_o)
    subs = [w // LANES for w in WIDTHS]
    offs = [sum(subs[:c]) for c in range(len(subs))]

    barrier = pltpu.get_barrier_semaphore()
    for dev in (partner, xdev, ydev):
        pl.semaphore_signal(barrier, inc=1, device_id={"ep": dev}, device_id_type=MESH)

    def h_copy(e):
        return pltpu.make_async_copy(h_hbm.at[e], h.at[e], h_sem.at[e])

    def wd_copy(c, e):
        slot = lax.rem(c * n_exp + e, 3)
        return pltpu.make_async_copy(wd_hbm.at[e, :, pl.ds(offs[c] * LANES, WIDTHS[c])], wd.at[slot, :, pl.ds(0, WIDTHS[c])], wd_sem.at[slot])

    h_copy(0).start()
    wd_copy(0, 0).start()
    wd_copy(0, 1).start()
    for e in range(1, n_exp):
        h_copy(e).start()
    ybuf[pl.ds(n_exp * cap * SUB, 8), :] = jnp.zeros((8, LANES), jnp.float32)
    pl.semaphore_wait(barrier, 3)

    def remote(src, dst, send, recv, dev):
        return pltpu.make_async_remote_copy(src_ref=src, dst_ref=dst, send_sem=send, recv_sem=recv, device_id={"ep": dev}, device_id_type=MESH)

    def full(c):
        return pl.ds(offs[c] * tok_dev, subs[c] * tok_dev)

    def low(c):
        return pl.ds(offs[c] * tok_dev, subs[c] * half)

    def high(c):
        return pl.ds(offs[c] * tok_dev + subs[c] * half, subs[c] * half)

    def land(c):
        return pl.ds(offs[c] * half, subs[c] * half)

    def core_copy(c, i):
        return remote(part.at[2 * chips[i] + 1 - core, pl.ds(0, subs[c] * tok_dev)], sums.at[chips[i], full(c)], send_core.at[c, i], recv_core.at[c, i], partner)

    def x_copy(c, i):
        return remote(sums.at[(chip_d, chip_x)[i], low(c)], got_x.at[i, land(c)], send_x.at[c, i], recv_x.at[c, i], xdev)

    def y_copy(c, i):
        return remote(sums.at[(chip_d, chip_y)[i], high(c)], got_y.at[i, land(c)], send_y.at[c, i], recv_y.at[c, i], ydev)

    def hop_copy(c, i):
        if i == 0:
            return remote(sums.at[chip_y, low(c)], got_2.at[0, land(c)], send_2.at[c, 0], recv_2.at[c, 0], ydev)
        return remote(sums.at[chip_x, high(c)], got_2.at[1, land(c)], send_2.at[c, 1], recv_2.at[c, 1], xdev)

    def add_into(dst, src, n):
        def one(i, _):
            at = pl.ds(pl.multiple_of(i * 128, 128), 128)
            dst[at, :] = dst[at, :] + src[at, :]
            return 0
        lax.fori_loop(0, n // 128, one, 0)

    def on_core(c, i):
        core_copy(c, i).wait_recv()
        add_into(sums.at[chips[i], full(c)], part.at[2 * chips[i] + core, pl.ds(0, subs[c] * tok_dev)], subs[c] * tok_dev)
        if i == 0:
            x_copy(c, 0).start()
            y_copy(c, 0).start()
        elif i == 1:
            x_copy(c, 1).start()
        elif i == 2:
            y_copy(c, 1).start()

    def on_first(c):
        x_copy(c, 0).wait_recv()
        add_into(sums.at[chip_y, low(c)], got_x.at[0, land(c)], subs[c] * half)
        hop_copy(c, 0).start()
        y_copy(c, 0).wait_recv()
        add_into(sums.at[chip_x, high(c)], got_y.at[0, land(c)], subs[c] * half)
        hop_copy(c, 1).start()

    def on_own(c):
        x_copy(c, 1).wait_recv()
        add_into(sums.at[chip_o, low(c)], got_x.at[1, land(c)], subs[c] * half)
        y_copy(c, 1).wait_recv()
        add_into(sums.at[chip_o, high(c)], got_y.at[1, land(c)], subs[c] * half)

    def finish(c):
        hop_copy(c, 0).wait_recv()
        add_into(sums.at[chip_o, low(c)], got_2.at[0, land(c)], subs[c] * half)
        hop_copy(c, 1).wait_recv()
        add_into(sums.at[chip_o, high(c)], got_2.at[1, land(c)], subs[c] * half)
        for i in range(subs[c]):
            at = (offs[c] + i) * LANES
            out_ref[:, at:at + LANES] = sums[chip_o, pl.ds(offs[c] * tok_dev + i, tok_dev, stride=subs[c]), :]

    def down(c, lo, hi):
        width = WIDTHS[c]

        def one(e, _):
            slot = lax.rem(c * n_exp + e, 3)
            @pl.when(e + 2 < n_exp)
            def _():
                wd_copy(c, e + 2).start()
            if c + 1 < len(WIDTHS):
                @pl.when(e + 2 >= n_exp)
                def _():
                    wd_copy(c + 1, e + 2 - n_exp).start()
            if c == 0:
                h_copy(e).wait()
            wd_copy(c, e).wait()
            y = jnp.dot(h[e], wd[slot, :, 0:width], preferred_element_type=jnp.float32)
            y = y.astype(jnp.bfloat16).astype(jnp.float32)
            gate = gate_ref[e]
            for i in range(subs[c]):
                ybuf[pl.ds(e * (cap * SUB) + i, cap, stride=SUB), :] = y[:, i * LANES:(i + 1) * LANES] * gate
            return 0
        lax.fori_loop(lo, hi, one, 0)

    def combine(c, i):
        sub = subs[c]

        def one_dev(j, _):
            dev = 2 * chips[i] + j

            def one(b, _):
                at = dev * (8 * tok_dev) + b * 8
                for u in range(8):
                    acc = None
                    for k in range(TOP):
                        table = slot_ref.at[pl.ds(k * tok_dev + u, slot_ref.shape[0] - TOP * tok_dev)]
                        row = ybuf[pl.ds(table[at], sub), :]
                        acc = row if acc is None else acc + row
                    part[dev, pl.ds(b * (8 * sub) + u * sub, sub), :] = acc
                return 0
            lax.fori_loop(0, tok_dev // 8, one, 0)
            return 0
        lax.fori_loop(0, 2, one_dev, 0)

    last = len(WIDTHS) - 1
    for c in range(len(WIDTHS)):
        down(c, 0, 1)
        if c >= 1:
            on_core(c - 1, 3)
        down(c, 1, n_exp // 2)
        if c >= 1:
            on_first(c - 1)
        down(c, n_exp // 2, n_exp)
        if c >= 2:
            on_own(c - 2)
            finish(c - 2)
        for i in range(4):
            if c >= 1:
                core_copy(c - 1, i).wait_send()
            combine(c, i)
            core_copy(c, i).start()
            if i >= 1:
                on_core(c, i - 1)
    on_core(last, 3)
    on_first(last)
    on_own(last - 1)
    finish(last - 1)
    on_own(last)
    finish(last)
    for c in range(len(WIDTHS)):
        for i in range(2):
            x_copy(c, i).wait_send()
            y_copy(c, i).wait_send()
            hop_copy(c, i).wait_send()
    for i in range(4):
        core_copy(last, i).wait_send()


def down_reduce(slot_off, hidden, w_down, gate_col, tok_dev):
    n_exp, cap, inter = hidden.shape
    d = w_down.shape[2]
    n_chunk = len(WIDTHS)
    rows = tok_dev * d // LANES
    f32 = jnp.float32
    return pl.pallas_call(
        down_kernel,
        out_shape=jax.ShapeDtypeStruct((tok_dev, d), f32),
        in_specs=[
            pl.BlockSpec(memory_space=pltpu.SMEM),
            pl.BlockSpec(memory_space=pl.ANY),
            pl.BlockSpec(memory_space=pl.ANY),
            pl.BlockSpec(memory_space=pltpu.VMEM),
        ],
        out_specs=pl.BlockSpec(memory_space=pltpu.VMEM),
        scratch_shapes=[
            pltpu.VMEM((n_exp, cap, inter), jnp.bfloat16),
            pltpu.VMEM((3, inter, max(WIDTHS)), jnp.bfloat16),
            pltpu.VMEM((n_exp * cap * SUB + 8, LANES), f32),
            pltpu.VMEM((8, tok_dev * SUB, LANES), f32),
            pltpu.VMEM((4, rows, LANES), f32),
            pltpu.VMEM((2, rows // 2, LANES), f32),
            pltpu.VMEM((2, rows // 2, LANES), f32),
            pltpu.VMEM((2, rows // 2, LANES), f32),
            pltpu.SemaphoreType.DMA((n_exp,)),
            pltpu.SemaphoreType.DMA((3,)),
            pltpu.SemaphoreType.DMA((n_chunk, 4)),
            pltpu.SemaphoreType.DMA((n_chunk, 4)),
            pltpu.SemaphoreType.DMA((n_chunk, 2)),
            pltpu.SemaphoreType.DMA((n_chunk, 2)),
            pltpu.SemaphoreType.DMA((n_chunk, 2)),
            pltpu.SemaphoreType.DMA((n_chunk, 2)),
            pltpu.SemaphoreType.DMA((n_chunk, 2)),
            pltpu.SemaphoreType.DMA((n_chunk, 2)),
        ],
        compiler_params=pltpu.CompilerParams(vmem_limit_bytes=VMEM_LIMIT, collective_id=1, has_side_effects=True),
        cost_estimate=pl.CostEstimate(flops=2 * n_exp * cap * d * inter, bytes_accessed=2 * n_exp * d * inter, transcendentals=0),
        name="down_reduce",
    )(slot_off, hidden, w_down, gate_col)


def solution(mesh):
    n_dev = mesh.shape["ep"]

    def local_block(hidden_in, norm_gain, router_w, w_gate, w_up, w_down, ws_gate, ws_up, ws_down, expert_ids):
        n_exp = w_gate.shape[0]
        cap = 512
        ids_t = jnp.pad(expert_ids.T, ((0, 8 - TOP), (0, 0)), constant_values=-1)
        xn_all, base, tok_off, slots, gate_col = gather_rows(hidden_in, norm_gain[None, :], router_w, ids_t, ws_gate, ws_up, ws_down, n_dev, n_exp, cap)
        hidden = gate_up(tok_off.reshape(-1), xn_all, w_gate, w_up)
        routed = down_reduce(slots.reshape(-1), hidden, w_down, gate_col, hidden_in.shape[0])
        return (base + routed).astype(jnp.bfloat16)

    row_spec = P(("dp", "ep"), None)
    in_specs = (row_spec, P(), P(), P("ep"), P("ep"), P("ep"), P(), P(), P(), row_spec)
    return jax.shard_map(local_block, mesh=mesh, in_specs=in_specs, out_specs=row_spec, check_vma=False)
```
